32 devices in a mesh: section: 8 (over z, y), expert: 4 (over x, core).
Axes of the slice: x: 2, y: 2, z: 4, core: 2. Of those that a mesh axis runs over, the one named last changes fastest.
Arguments:
- grad_out: bfloat16 [8, 512, 3584], P('section', 'expert'), may hold values from -6 to 6
- hidden_act: bfloat16 [8, 512, 1024], P('section', 'expert'), may hold values from -0.29882812 to 0.29882812
- scores: float32 [8, 512, 4], P('section', 'expert'), may hold values from -8 to 8
- expert_ids: int32 [8, 512], P('section', 'expert'), may hold values from 0 to 3, as said below
- slot_ids: int32 [8, 512], P('section', 'expert'), may hold values from 0 to 55, as said below
- counts: int32 [8, 4, 4], P('section'), may hold values from 0 to 56, as said below
- down_weight: bfloat16 [4, 1024, 3584], P('expert'), may hold values from -0.1875 to 0.1875
- router: bfloat16 [4, 3584], replicated, may hold values from -0.8984375 to 0.8984375
Outputs:
- act_grad: bfloat16 [8, 512, 1024], P('section', 'expert')
- score_grad: float32 [8, 512, 4], P('section', 'expert')
- upstream_grad: bfloat16 [8, 512, 3584], P('section', 'expert')
The draws below stay inside these ranges and needn't reach their ends.
Inputs may be any that keep to these rules, and one draw needn't show every extreme that they name: `expert_ids`: the 128 tokens of one device name each expert at most 56 times; in every section one expert gets exactly 56 tokens from every device. `slot_ids`: a token's slot is the number of earlier tokens of its device that name the same expert. counts[s, e] is at most the number of tokens of device s of the section that name expert e, and may be smaller; routes whose slot is not below it are dropped; for the expert that gets 56 tokens from every device it is 56.
All inputs are finite; a program needn't handle non-finite values.
Results may differ from the reference program's by a relative error of at most 0.009.
Values may be sent and summed in bfloat16 or wider, within the bound.
A program may use at most 64 MiB of HBM per device.

```python
import jax
import jax.numpy as jnp
from jax import lax

D = 3584
FF = 1024
TOK_DEV = 128
TOKENS = 512
EXPERT_TOTAL = 4
SLOT_LIMIT = 56
N_SECTION = 8
N_EXPERT = 4


def route_table(key):
    base = jax.random.fold_in(key, 7)
    keys = jax.random.split(base, 5)
    block_list = N_SECTION * N_EXPERT
    hottest = jax.random.randint(keys[0], (N_SECTION,), 0, EXPERT_TOTAL)
    level_values = jax.random.randint(keys[1], (N_SECTION, EXPERT_TOTAL), 0, 4)
    expert_range = jnp.arange(EXPERT_TOTAL, dtype=jnp.int32)
    busiest_flag = expert_range[None, :] == hottest[:, None]
    extra_score = level_values * 2048 + jnp.where(busiest_flag, 1 << 20, 0)
    extra_score = jnp.repeat(extra_score, N_EXPERT, axis=0)
    random_jitter = jax.random.randint(keys[2], (block_list, EXPERT_TOTAL, SLOT_LIMIT), 0, 4096)
    sorted_order = (extra_score[:, :, None] + random_jitter).reshape(block_list, EXPERT_TOTAL * SLOT_LIMIT).astype(jnp.int32)
    unused, picked = lax.top_k(sorted_order, TOK_DEV)
    chosen = (picked // SLOT_LIMIT).astype(jnp.int32)
    perm_keys = jax.random.split(keys[3], block_list)
    orders = jax.vmap(lambda one_key: jax.random.permutation(one_key, TOK_DEV))(perm_keys)
    chosen = jnp.take_along_axis(chosen, orders, axis=1)
    same = chosen[:, :, None] == chosen[:, None, :]
    positions = jnp.arange(TOK_DEV, dtype=jnp.int32)
    earlier = positions[None, :] < positions[:, None]
    places = jnp.sum(jnp.where(same & earlier[None, :, :], 1, 0), axis=2).astype(jnp.int32)
    tallies = jnp.sum(jnp.where(chosen[:, :, None] == expert_range[None, None, :], 1, 0), axis=1).astype(jnp.int32)
    tallies = tallies.reshape(N_SECTION, N_EXPERT, EXPERT_TOTAL)
    lowest = max(1, SLOT_LIMIT // 2)
    limits = jax.random.randint(keys[4], (N_SECTION, N_EXPERT, EXPERT_TOTAL), lowest, SLOT_LIMIT + 1).astype(jnp.int32)
    limits = jnp.where(busiest_flag[:, None, :], SLOT_LIMIT, limits).astype(jnp.int32)
    accepted = jnp.minimum(tallies, limits).astype(jnp.int32)
    return (chosen.reshape(N_SECTION, TOKENS), places.reshape(N_SECTION, TOKENS), accepted)


def draw_expert_ids(key, part):
    return route_table(key)[0]


def draw_slot_ids(key, part):
    return route_table(key)[1]


def draw_counts(key, part):
    return route_table(key)[2]


def level_of(own_key, shape, shards, smallest, largest):
    level = 1.0
    for axis_at, parts in shards:
        steps = jax.random.uniform(jax.random.fold_in(jax.random.fold_in(own_key, 6), axis_at), (parts,), jnp.float32, smallest / len(shards), largest / len(shards))
        level = level * jnp.repeat(jnp.exp(steps), shape[axis_at] // parts).reshape((-1,) + (1,) * (len(shape) - 1 - axis_at))
    return level


def normal_values(stream_key, shape, scale, most, pieces=(), held_as=jnp.bfloat16):
    result = scale * jax.random.normal(stream_key, shape, jnp.float32)
    if pieces:
        result = result * level_of(stream_key, shape, pieces, -0.22, 0.18)
    return jnp.clip(result, -most, most).astype(held_as)


def setup_inputs(seed: int = 0) -> dict:
    seeds = jax.random.split(jax.random.key(seed), 9)
    return {
        "grad_out": normal_values(seeds[0], (N_SECTION, TOKENS, D), 1.0, 6.0, ((0, 8), (1, 4))),
        "hidden_act": normal_values(seeds[1], (N_SECTION, TOKENS, FF), 0.05, 0.29882812, ((0, 8), (1, 4))),
        "scores": normal_values(seeds[2], (N_SECTION, TOKENS, EXPERT_TOTAL), 1.5, 8.0, ((0, 8), (1, 4)), jnp.float32),
        "expert_ids": draw_expert_ids(jax.random.fold_in(seeds[8], 71), 0),
        "slot_ids": draw_slot_ids(jax.random.fold_in(seeds[8], 71), 0),
        "counts": draw_counts(jax.random.fold_in(seeds[8], 71), 0),
        "down_weight": normal_values(seeds[6], (EXPERT_TOTAL, FF, D), FF ** -0.5, 0.1875, ((0, 4),)),
        "router": normal_values(seeds[7], (EXPERT_TOTAL, D), 0.15, 0.8984375),
    }


route_scale = 2.5


def one_section(pack, down_weight, router):
    grad_out, hidden_act, scores, expert_ids, slot_ids, counts = pack
    source = (jnp.arange(TOKENS) // TOK_DEV).astype(jnp.int32)
    own_limit = counts[source, expert_ids]
    is_live = slot_ids < own_limit
    onehot = expert_ids[:, None] == jnp.arange(EXPERT_TOTAL, dtype=jnp.int32)[None, :]
    chosen_logit = jnp.sum(jnp.where(onehot, scores, 0.0), axis=1)
    sigmoid_vals = jax.nn.sigmoid(chosen_logit)
    gate_bf = (route_scale * sigmoid_vals).astype(jnp.bfloat16)
    masked = jnp.where(is_live[:, None], grad_out, jnp.zeros_like(grad_out))
    slot_total = N_EXPERT * SLOT_LIMIT
    target = (expert_ids * slot_total + source * SLOT_LIMIT + slot_ids).astype(jnp.int32)
    buffer = jnp.zeros((EXPERT_TOTAL * slot_total, D), jnp.bfloat16).at[target].set(masked, mode="drop")
    buffer = buffer.reshape(EXPERT_TOTAL, slot_total, D)

    def expert_back(pair):
        rows_in, weight = pair
        return jnp.dot(rows_in, weight.T, preferred_element_type=jnp.float32)

    back_rows = lax.map(expert_back, (buffer, down_weight)).reshape(EXPERT_TOTAL * slot_total, FF)
    safe_target = jnp.where(is_live, target, 0).astype(jnp.int32)
    own_back = jnp.where(is_live[:, None], back_rows[safe_target], 0.0)
    act_grad = (gate_bf.astype(jnp.float32)[:, None] * own_back).astype(jnp.bfloat16)
    route_grad = jnp.sum(hidden_act.astype(jnp.float32) * own_back, axis=1)
    slope_term = route_grad * route_scale * sigmoid_vals * (1.0 - sigmoid_vals)
    score_grad = jnp.where(onehot, slope_term[:, None], 0.0)
    score_bf = score_grad.astype(jnp.bfloat16)
    token_grad = (grad_out.astype(jnp.float32) + jnp.dot(score_bf, router, preferred_element_type=jnp.float32)).astype(jnp.bfloat16)
    return act_grad, score_grad, token_grad


def reference(grad_out, hidden_act, scores, expert_ids, slot_ids, counts, down_weight, router):
    def per_section(pack):
        return one_section(pack, down_weight, router)

    act_grad, score_grad, token_grad = lax.map(per_section, (grad_out, hidden_act, scores, expert_ids, slot_ids, counts))
    upstream_grad = jnp.concatenate([token_grad[1:], jnp.zeros_like(token_grad[:1])], axis=0)
    return (act_grad, score_grad, upstream_grad)
```

```python
import functools

import jax
import jax.numpy as jnp
from jax import lax
from jax.experimental import pallas as pl
from jax.experimental.pallas import tpu as pltpu
from jax.sharding import PartitionSpec as P

route_scale = 2.5
MESH = pl.DeviceIdType.MESH
BF = jnp.bfloat16
F32 = jnp.float32


def row_parts(capacity):
    head = capacity // 16 * 16
    if head == capacity and head >= 32:
        head -= 16
    parts = []
    if head > 16:
        parts.append((0, head - 16, head - 16))
    if head:
        parts.append((max(head - 16, 0), head, 16))
    if capacity > head:
        parts.append((head, capacity, -(-(capacity - head) // 8) * 8))
    return parts


def column_cuts(width, pieces):
    while width % (pieces * 128):
        pieces -= 1
    return pieces, width // pieces


def kernel(cfg, *refs):
    n_parts = len(cfg["parts"])
    counts = [count for count, _ in cfg["cuts"]]
    sizes = [6, counts[0], cfg["weight_cuts"][0], 4, n_parts, n_parts, n_parts] + counts
    pl.run_scoped(
        lambda *sems: exchange(cfg, refs[:8], refs[8:13], refs[13:], sems),
        *[pltpu.SemaphoreType.DMA((size,)) for size in sizes])


def exchange(cfg, inputs, outputs, scratch, sems):
    grad_hbm, hidden_hbm, logits_hbm, ids_hbm, slots_hbm, counts_hbm, weight_hbm, router_hbm = inputs
    act_ref, score_ref, got, got_slope, router_ref = outputs
    n, n_section, parts, cuts = cfg["n"], cfg["n_section"], cfg["parts"], cfg["cuts"]
    n_parts = len(parts)
    rest = list(scratch)
    take = lambda count: [rest.pop(0) for _ in range(count)]
    grad, hidden, weight, slope_out = take(4)
    logits_ref, ids_ref, slots_ref, counts_ref = take(4)
    sends, recvs, accs, results, returns, hiddens = (take(n_parts) for _ in range(6))
    load_sem, grad_sem, weight_sem, up_sem, send_sem, back_send, back_recv = sems[:7]
    recv_sems = sems[7:]

    tok, width = grad.shape
    section = lax.axis_index("section")
    me = lax.axis_index("expert")
    chips = n // 2
    chip, core = me // 2, lax.rem(me, 2)

    def peer(k, sign):
        far = k // 2
        return 2 * lax.rem(chip + chips + sign * far, chips) + (k % 2 if far else lax.rem(core + k, 2))

    def landing(k):
        return 2 * (k // 2) + core if k // 2 else k

    target = [peer(k, 1) for k in range(n)]
    source = [peer(k, -1) for k in range(n)]
    early = [k for k in range(2, n) if k % 2 == 0]
    late = [k for k in range(2, n) if k % 2] + [1]
    has_prev, has_next = section > 0, section < n_section - 1

    pairs = [
        (ids_hbm, ids_ref), (slots_hbm, slots_ref), (counts_hbm.at[0], counts_ref),
        (logits_hbm.at[0], logits_ref), (router_hbm, router_ref), (hidden_hbm.at[0], hidden),
    ]
    loads = [pltpu.make_async_copy(src, dst, load_sem.at[i]) for i, (src, dst) in enumerate(pairs)]
    grad_loads = [
        pltpu.make_async_copy(
            grad_hbm.at[0, :, pl.ds(c * cuts[0][1], cuts[0][1])],
            grad.at[:, pl.ds(c * cuts[0][1], cuts[0][1])],
            grad_sem.at[c],
        )
        for c in range(cuts[0][0])
    ]
    for load in loads[:3] + grad_loads + loads[3:]:
        load.start()
    weight_cuts, weight_cols = cfg["weight_cuts"]
    weight_loads = [
        pltpu.make_async_copy(
            weight_hbm.at[0, :, pl.ds(c * weight_cols, weight_cols)],
            weight.at[:, pl.ds(c * weight_cols, weight_cols)],
            weight_sem.at[c],
        )
        for c in range(weight_cuts)
    ]

    barrier = pltpu.get_barrier_semaphore()
    for k in range(1, n):
        pl.semaphore_signal(barrier, inc=1, device_id=(section, target[k]), device_id_type=MESH)

    @pl.when(has_prev)
    def _():
        pl.semaphore_signal(barrier, inc=1, device_id=(section - 1, me), device_id_type=MESH)

    @pl.when(has_next)
    def _():
        pl.semaphore_signal(barrier, inc=1, device_id=(section + 1, me), device_id_type=MESH)

    for load in loads[:3]:
        load.wait()
    chosen = ids_ref[...]
    places = slots_ref[...]
    limit = jnp.zeros_like(chosen)
    slot_of = jnp.zeros_like(chosen)
    for k in range(n):
        here = chosen == target[k]
        limit = jnp.where(here, counts_ref[me, target[k]], limit)
        slot_of = jnp.where(here, k, slot_of)
    live = places < limit
    picks = []
    for low, high, padded in parts:
        inside = live & (places >= low) & (places < high)
        goal = jnp.where(inside, slot_of * padded + places - low, -1)
        picks.append(lax.broadcasted_iota(jnp.int32, (n * padded, tok), 0) == goal)
    eye = lax.broadcasted_iota(jnp.int32, (tok, tok), 0) == lax.broadcasted_iota(jnp.int32, (tok, tok), 1)

    grad_up = pltpu.make_async_remote_copy(
        src_ref=grad, dst_ref=got, send_sem=up_sem.at[0], recv_sem=up_sem.at[1],
        device_id=(section - 1, me), device_id_type=MESH)
    slope_up = pltpu.make_async_remote_copy(
        src_ref=slope_out, dst_ref=got_slope, send_sem=up_sem.at[2], recv_sem=up_sem.at[3],
        device_id=(section - 1, me), device_id_type=MESH)

    def dispatch(p, k, span, sem):
        return pltpu.make_async_remote_copy(
            src_ref=sends[p].at[k, :, span], dst_ref=recvs[p].at[landing(k), :, span],
            send_sem=send_sem.at[p], recv_sem=sem,
            device_id=(section, target[k]), device_id_type=MESH)

    def give_back(p, k):
        return pltpu.make_async_remote_copy(
            src_ref=results[p].at[k], dst_ref=returns[p].at[landing(k)],
            send_sem=back_send.at[p], recv_sem=back_recv.at[p],
            device_id=(section, source[k]), device_id_type=MESH)

    def all_of(src, dst, send, recv):
        return pltpu.make_async_remote_copy(
            src_ref=src, dst_ref=dst, send_sem=send, recv_sem=recv,
            device_id=(section, target[1]), device_id_type=MESH)

    others = pl.ds(1, n - 1)
    barred = True
    for p, (low, high, padded) in enumerate(parts):
        count, cols = cuts[p]
        pick = picks[p].astype(BF)
        for c in range(count):
            span = pl.ds(c * cols, cols)
            if p == 0:
                grad_loads[c].wait()
            block = jnp.dot(pick, grad[:, span], preferred_element_type=F32).astype(BF)
            block = block.reshape(n, padded, cols)
            sends[p][:, :, span] = block
            recvs[p][0, :, span] = block[0]
            if barred:
                pl.semaphore_wait(barrier, n - 1 + jnp.where(has_prev, 1, 0) + jnp.where(has_next, 1, 0))
                barred = False
            for k in early + late:
                dispatch(p, k, span, recv_sems[p].at[c]).start()
        if p == 0:

            @pl.when(has_prev)
            def _():
                grad_up.start()

            for load in weight_loads:
                load.start()

    def upright(row):
        return jnp.sum(jnp.where(eye, row, 0), axis=1, keepdims=True)

    for load in loads[3:]:
        load.wait()
    logits = logits_ref[...]
    onehot = chosen == lax.broadcasted_iota(jnp.int32, logits.shape, 0)
    chosen_logit = jnp.sum(jnp.where(onehot, logits, 0.0), axis=0, keepdims=True)
    sigmoid_vals = jax.nn.sigmoid(chosen_logit)
    gate = upright((route_scale * sigmoid_vals).astype(BF).astype(F32))
    for p in range(n_parts):
        hiddens[p][...] = jnp.dot(picks[p].astype(BF), hidden[...], preferred_element_type=F32)

    weights_waited = 0
    held = []
    for p, (low, high, padded) in enumerate(parts):
        count, cols = cuts[p]
        rows = n * padded
        for c in range(count):
            while weights_waited * weight_cols < (c + 1) * cols:
                weight_loads[weights_waited].wait()
                weights_waited += 1
            span = pl.ds(c * cols, cols)
            all_of(sends[p].at[others, :, span], recvs[p].at[others, :, span],
                   send_sem.at[p], recv_sems[p].at[c]).wait_recv()
            part = lax.dot_general(
                recvs[p][:, :, span].reshape(rows, cols), weight[:, span],
                (((1,), (1,)), ((), ())), preferred_element_type=F32)
            if c:
                part = accs[p][...] + part
            if c < count - 1:
                accs[p][...] = part
        done = part.astype(BF).reshape(n, padded, part.shape[1])
        results[p][...] = done
        returns[p][0] = done[0]
        for k in early:
            give_back(p, k).start()
        held += [(p, k) for k in late]
        if p in (0, n_parts - 1):
            for q, k in held:
                give_back(q, k).start()
            held = []

    route_grad = jnp.zeros((1, tok), F32)
    for p, (low, high, padded) in enumerate(parts):
        rows = n * padded
        all_of(results[p].at[others], returns[p].at[others], back_send.at[p], back_recv.at[p]).wait_recv()
        own = returns[p][...].reshape(rows, returns[p].shape[2]).astype(F32)
        by_row = jnp.sum(hiddens[p][...] * own, axis=1, keepdims=True)
        route_grad += jnp.sum(jnp.where(picks[p], by_row, 0.0), axis=0, keepdims=True)
    slope = route_grad * route_scale * sigmoid_vals * (1.0 - sigmoid_vals)
    slopes = jnp.where(onehot, slope, 0.0)
    slope_out[...] = slopes

    @pl.when(has_prev)
    def _():
        slope_up.start()

    score_ref[0] = slopes
    own_back = None
    for p, (low, high, padded) in enumerate(parts):
        rows = n * padded
        term = lax.dot_general(
            picks[p].astype(BF), returns[p][...].reshape(rows, returns[p].shape[2]),
            (((0,), (0,)), ((), ())), preferred_element_type=F32)
        own_back = term if own_back is None else own_back + term
    act_ref[0] = (gate * own_back).astype(BF)

    for p in range(n_parts):
        all_of(sends[p].at[others], recvs[p].at[others], send_sem.at[p], recv_sems[p].at[0]).wait_send()
        all_of(results[p].at[others], returns[p].at[others], back_send.at[p], back_recv.at[p]).wait_send()

    @pl.when(has_prev)
    def _():
        grad_up.wait_send()
        slope_up.wait_send()

    @pl.when(has_next)
    def _():
        grad_up.wait_recv()
        slope_up.wait_recv()


def finish_kernel(cfg, act_in, score_in, got, got_slope, router_ref, act_out, score_out, up_out, up):
    def scoped(sems):
        count, cols = cfg["final_cuts"]
        copies = [pltpu.make_async_copy(act_in, act_out, sems.at[0]),
                  pltpu.make_async_copy(score_in, score_out, sems.at[1]),
                  pltpu.make_async_copy(up, up_out.at[0], sems.at[2])]
        for copy in copies[:2]:
            copy.start()
        is_last = lax.axis_index("section") == cfg["n_section"] - 1
        scores_bf = got_slope[...].astype(BF)
        for c in range(count):
            span = pl.ds(c * cols, cols)
            term = lax.dot_general(
                scores_bf, router_ref[:, span], (((0,), (0,)), ((), ())), preferred_element_type=F32)
            token_grad = got[:, span].astype(F32) + term
            up[:, span] = jnp.where(is_last, 0.0, token_grad).astype(BF)
            pltpu.make_async_copy(up.at[:, span], up_out.at[0, :, span], sems.at[2]).start()
        for copy in copies:
            copy.wait()

    pl.run_scoped(scoped, pltpu.SemaphoreType.DMA((3,)))


def on_device(grad_out, hidden_act, scores, expert_ids, slot_ids, counts, down_weight, router):
    n, n_section = lax.axis_size("expert"), lax.axis_size("section")
    _, tok, width = grad_out.shape
    hidden_width = hidden_act.shape[2]
    experts = scores.shape[2]
    capacity = max(2, 7 * tok // (4 * n))
    parts = row_parts(capacity)
    cuts = [column_cuts(width, 2 if low and padded >= 16 else 4) for low, _, padded in parts]
    cfg = dict(n=n, n_section=n_section, parts=parts, cuts=cuts, weight_cuts=column_cuts(width, 4),
               final_cuts=column_cuts(width, 7))
    hbm = pl.BlockSpec(memory_space=pltpu.HBM)
    vmem = pl.BlockSpec(memory_space=pltpu.VMEM)
    scratch = [
        pltpu.VMEM((tok, width), BF),
        pltpu.VMEM((tok, hidden_width), BF),
        pltpu.VMEM((hidden_width, width), BF),
        pltpu.VMEM((experts, tok), F32),
        pltpu.VMEM((experts, tok), F32),
        pltpu.VMEM((1, tok), jnp.int32),
        pltpu.VMEM((1, tok), jnp.int32),
        pltpu.SMEM(counts.shape[1:], jnp.int32),
    ]
    scratch += [pltpu.VMEM((n, padded, width), BF) for _, _, padded in parts]
    scratch += [pltpu.VMEM((n, padded, width), BF) for _, _, padded in parts]
    scratch += [pltpu.VMEM((n * padded, hidden_width), F32) for _, _, padded in parts]
    scratch += [pltpu.VMEM((n, padded, hidden_width), BF) for _, _, padded in parts]
    scratch += [pltpu.VMEM((n, padded, hidden_width), BF) for _, _, padded in parts]
    scratch += [pltpu.VMEM((n * padded, hidden_width), F32) for _, _, padded in parts]
    kept = 2 * tok * (hidden_width + width) + 8 * tok * experts + 2 * experts * width
    vmem_limit = (67043328 - kept - 128 * 1024) // 4096 * 4096
    held = pl.pallas_call(
        functools.partial(kernel, cfg),
        out_shape=(
            pltpu.VMEM((1, tok, hidden_width), BF),
            pltpu.VMEM((1, experts, tok), F32),
            pltpu.VMEM((tok, width), BF),
            pltpu.VMEM((experts, tok), F32),
            pltpu.VMEM(router.shape, BF),
        ),
        in_specs=[hbm] * 8,
        out_specs=(vmem,) * 5,
        scratch_shapes=scratch,
        compiler_params=pltpu.CompilerParams(
            collective_id=0, has_side_effects=True, vmem_limit_bytes=vmem_limit),
    )(grad_out, hidden_act, jnp.swapaxes(scores, 1, 2), expert_ids, slot_ids, counts, down_weight, router)
    act_grad, score_grad, upstream = pl.pallas_call(
        functools.partial(finish_kernel, cfg),
        out_shape=(
            jax.ShapeDtypeStruct((1, tok, hidden_width), BF),
            jax.ShapeDtypeStruct((1, experts, tok), F32),
            jax.ShapeDtypeStruct((1, tok, width), BF),
        ),
        in_specs=[vmem] * 5,
        out_specs=(hbm,) * 3,
        scratch_shapes=[pltpu.VMEM((tok, width), BF)],
        compiler_params=pltpu.CompilerParams(vmem_limit_bytes=16 * 1024 * 1024),
    )(*held)
    return act_grad, jnp.swapaxes(score_grad, 1, 2), upstream


def solution(mesh):
    in_specs = (
        P("section", "expert", None),
        P("section", "expert", None),
        P("section", "expert", None),
        P("section", "expert"),
        P("section", "expert"),
        P("section", None, None),
        P("expert", None, None),
        P(),
    )
    out_specs = (
        P("section", "expert", None),
        P("section", "expert", None),
        P("section", "expert", None),
    )
    return jax.shard_map(
        on_device, mesh=mesh, in_specs=in_specs, out_specs=out_specs, check_vma=False
    )
```

```python
import functools

import jax
import jax.numpy as jnp
from jax import lax
from jax.experimental import pallas as pl
from jax.experimental.pallas import tpu as pltpu
from jax.sharding import PartitionSpec as P

route_scale = 2.5
MESH = pl.DeviceIdType.MESH
BF = jnp.bfloat16
F32 = jnp.float32


def row_parts(capacity):
    head = capacity // 16 * 16
    if head == capacity and head >= 32:
        head -= 16
    parts = [(0, head, head)] if head else []
    if capacity > head:
        parts.append((head, capacity, -(-(capacity - head) // 8) * 8))
    return parts


def row_pieces(parts):
    pieces = []
    for p, (low, high, padded) in enumerate(parts):
        edges = [0, 16, padded] if p == 0 and len(parts) > 1 and padded > 16 else [0, padded]
        pieces += [(p, first, last) for first, last in zip(edges[:-1], edges[1:])]
    return pieces


def column_cuts(width, pieces):
    while width % (pieces * 128):
        pieces -= 1
    return pieces, width // pieces


def kernel(cfg, *refs):
    n_parts, n_pieces = len(cfg["parts"]), len(cfg["pieces"])
    counts = [count for count, _ in cfg["cuts"]]
    sizes = [6, counts[0], cfg["weight_cuts"][0], 4, n_parts, n_pieces, n_pieces] + counts
    pl.run_scoped(
        lambda *sems: exchange(cfg, refs[:8], refs[8:13], refs[13:], sems),
        *[pltpu.SemaphoreType.DMA((size,)) for size in sizes])


def exchange(cfg, inputs, outputs, scratch, sems):
    grad_hbm, hidden_hbm, logits_hbm, ids_hbm, slots_hbm, counts_hbm, weight_hbm, router_hbm = inputs
    act_ref, score_ref, got, got_slope, router_ref = outputs
    n, n_section, parts, cuts = cfg["n"], cfg["n_section"], cfg["parts"], cfg["cuts"]
    pieces = cfg["pieces"]
    n_parts, n_pieces = len(parts), len(pieces)
    rest = list(scratch)
    take = lambda count: [rest.pop(0) for _ in range(count)]
    grad, hidden, weight, slope_out = take(4)
    logits_ref, ids_ref, slots_ref, counts_ref = take(4)
    sends, recvs, accs = (take(n_parts) for _ in range(3))
    results, returns, hiddens = (take(n_pieces) for _ in range(3))
    load_sem, grad_sem, weight_sem, up_sem, send_sem, back_send, back_recv = sems[:7]
    recv_sems = sems[7:]

    tok, width = grad.shape
    section = lax.axis_index("section")
    me = lax.axis_index("expert")
    chips = n // 2
    chip, core = me // 2, lax.rem(me, 2)

    def peer(k, sign):
        far = k // 2
        return 2 * lax.rem(chip + chips + sign * far, chips) + (k % 2 if far else lax.rem(core + k, 2))

    def landing(k):
        return 2 * (k // 2) + core if k // 2 else k

    target = [peer(k, 1) for k in range(n)]
    source = [peer(k, -1) for k in range(n)]
    early = [k for k in range(2, n) if k % 2 == 0]
    late = [k for k in range(2, n) if k % 2]
    has_prev, has_next = section > 0, section < n_section - 1

    pairs = [
        (ids_hbm, ids_ref), (slots_hbm, slots_ref), (counts_hbm.at[0], counts_ref),
        (logits_hbm.at[0], logits_ref), (router_hbm, router_ref), (hidden_hbm.at[0], hidden),
    ]
    loads = [pltpu.make_async_copy(src, dst, load_sem.at[i]) for i, (src, dst) in enumerate(pairs)]
    grad_loads = [
        pltpu.make_async_copy(
            grad_hbm.at[0, :, pl.ds(c * cuts[0][1], cuts[0][1])],
            grad.at[:, pl.ds(c * cuts[0][1], cuts[0][1])],
            grad_sem.at[c],
        )
        for c in range(cuts[0][0])
    ]
    for load in loads[:3] + grad_loads[:1]:
        load.start()
    barrier = pltpu.get_barrier_semaphore()
    for k in range(1, n):
        pl.semaphore_signal(barrier, inc=1, device_id=(section, target[k]), device_id_type=MESH)

    @pl.when(has_next)
    def _():
        pl.semaphore_signal(barrier, inc=1, device_id=(section + 1, me), device_id_type=MESH)

    for load in grad_loads[1:] + loads[3:]:
        load.start()
    weight_cuts, weight_cols = cfg["weight_cuts"]
    weight_loads = [
        pltpu.make_async_copy(
            weight_hbm.at[0, :, pl.ds(c * weight_cols, weight_cols)],
            weight.at[:, pl.ds(c * weight_cols, weight_cols)],
            weight_sem.at[c],
        )
        for c in range(weight_cuts)
    ]

    for load in loads[:3]:
        load.wait()
    chosen = ids_ref[...]
    places = slots_ref[...]
    limit = jnp.zeros_like(chosen)
    slot_of = jnp.zeros_like(chosen)
    for k in range(n):
        here = chosen == target[k]
        limit = jnp.where(here, counts_ref[me, target[k]], limit)
        slot_of = jnp.where(here, k, slot_of)
    live = places < limit

    def picked(low, high, padded):
        inside = live & (places >= low) & (places < high)
        goal = jnp.where(inside, slot_of * padded + places - low, -1)
        return lax.broadcasted_iota(jnp.int32, (n * padded, tok), 0) == goal

    eye = lax.broadcasted_iota(jnp.int32, (tok, tok), 0) == lax.broadcasted_iota(jnp.int32, (tok, tok), 1)

    grad_up = pltpu.make_async_remote_copy(
        src_ref=grad, dst_ref=got, send_sem=up_sem.at[0], recv_sem=up_sem.at[1],
        device_id=(section - 1, me), device_id_type=MESH)
    slope_up = pltpu.make_async_remote_copy(
        src_ref=slope_out, dst_ref=got_slope, send_sem=up_sem.at[2], recv_sem=up_sem.at[3],
        device_id=(section - 1, me), device_id_type=MESH)

    def dispatch(p, k, span, sem):
        return pltpu.make_async_remote_copy(
            src_ref=sends[p].at[k, :, span], dst_ref=recvs[p].at[landing(k), :, span],
            send_sem=send_sem.at[p], recv_sem=sem,
            device_id=(section, target[k]), device_id_type=MESH)

    def give_back(q, k):
        return pltpu.make_async_remote_copy(
            src_ref=results[q].at[k], dst_ref=returns[q].at[landing(k)],
            send_sem=back_send.at[q], recv_sem=back_recv.at[q],
            device_id=(section, source[k]), device_id_type=MESH)

    def all_of(src, dst, send, recv):
        return pltpu.make_async_remote_copy(
            src_ref=src, dst_ref=dst, send_sem=send, recv_sem=recv,
            device_id=(section, target[1]), device_id_type=MESH)

    others = pl.ds(1, n - 1)
    barred = True
    for p, (low, high, padded) in enumerate(parts):
        count, cols = cuts[p]
        pick = picked(low, high, padded).astype(BF)
        for c in range(count):
            span = pl.ds(c * cols, cols)
            if p == 0:
                grad_loads[c].wait()
            block = jnp.dot(pick, grad[:, span], preferred_element_type=F32).astype(BF)
            block = block.reshape(n, padded, cols)
            sends[p][:, :, span] = block
            recvs[p][0, :, span] = block[0]
            if barred:
                pl.semaphore_wait(barrier, n - 1 + jnp.where(has_prev, 1, 0))
                barred = False
            for k in early + late + [1]:
                dispatch(p, k, span, recv_sems[p].at[c]).start()
        if p == 0:

            @pl.when(has_prev)
            def _():
                grad_up.start()

            for load in weight_loads:
                load.start()

    def upright(row):
        return jnp.sum(jnp.where(eye, row, 0), axis=1, keepdims=True)

    for load in loads[3:]:
        load.wait()
    logits = logits_ref[...]
    onehot = chosen == lax.broadcasted_iota(jnp.int32, logits.shape, 0)
    chosen_logit = jnp.sum(jnp.where(onehot, logits, 0.0), axis=0, keepdims=True)
    sigmoid_vals = jax.nn.sigmoid(chosen_logit)
    gate = upright((route_scale * sigmoid_vals).astype(BF).astype(F32))
    picks = [picked(parts[p][0] + first, parts[p][0] + last, last - first) for p, first, last in pieces]
    for q in range(n_pieces):
        hiddens[q][...] = jnp.dot(picks[q].astype(BF), hidden[...], preferred_element_type=F32)

    weights_waited = 0
    held = []
    for p, (low, high, padded) in enumerate(parts):
        count, cols = cuts[p]
        rows = n * padded
        for c in range(count):
            while weights_waited * weight_cols < (c + 1) * cols:
                weight_loads[weights_waited].wait()
                weights_waited += 1
            span = pl.ds(c * cols, cols)
            all_of(sends[p].at[others, :, span], recvs[p].at[others, :, span],
                   send_sem.at[p], recv_sems[p].at[c]).wait_recv()
            part = lax.dot_general(
                recvs[p][:, :, span].reshape(rows, cols), weight[:, span],
                (((1,), (1,)), ((), ())), preferred_element_type=F32)
            if c:
                part = accs[p][...] + part
            if c < count - 1:
                accs[p][...] = part
        done = part.astype(BF).reshape(n, padded, part.shape[1])
        for q, (of, first, last) in enumerate(pieces):
            if of == p:
                results[q][...] = done[:, first:last]
                returns[q][0] = done[0, first:last]
                give_back(q, 1).start()
                for k in early:
                    give_back(q, k).start()
                held += [(q, k) for k in late]
        rush = 1 if p < n_parts - 1 else n_pieces
        for q, k in [(q, k) for q, k in held if q < rush]:
            give_back(q, k).start()
        held = [(q, k) for q, k in held if q >= rush]

    route_grad = jnp.zeros((1, tok), F32)
    for q in range(n_pieces):
        all_of(results[q].at[others], returns[q].at[others], back_send.at[q], back_recv.at[q]).wait_recv()
        own = returns[q][...].reshape(hiddens[q].shape).astype(F32)
        by_row = jnp.sum(hiddens[q][...] * own, axis=1, keepdims=True)
        route_grad += jnp.sum(jnp.where(picks[q], by_row, 0.0), axis=0, keepdims=True)
    slope = route_grad * route_scale * sigmoid_vals * (1.0 - sigmoid_vals)
    slopes = jnp.where(onehot, slope, 0.0)
    slope_out[...] = slopes

    @pl.when(has_prev)
    def _():
        slope_up.start()

    score_ref[0] = slopes
    own_back = None
    for q in range(n_pieces):
        term = lax.dot_general(
            picks[q].astype(BF), returns[q][...].reshape(hiddens[q].shape),
            (((0,), (0,)), ((), ())), preferred_element_type=F32)
        own_back = term if own_back is None else own_back + term
    act_ref[0] = (gate * own_back).astype(BF)

    @pl.when(jnp.logical_not(has_next))
    def _():
        got[...] = jnp.zeros_like(got)
        got_slope[...] = jnp.zeros_like(got_slope)

    for p in range(n_parts):
        all_of(sends[p].at[others], recvs[p].at[others], send_sem.at[p], recv_sems[p].at[0]).wait_send()
    for q in range(n_pieces):
        all_of(results[q].at[others], returns[q].at[others], back_send.at[q], back_recv.at[q]).wait_send()

    @pl.when(has_prev)
    def _():
        grad_up.wait_send()
        slope_up.wait_send()

    @pl.when(has_next)
    def _():
        grad_up.wait_recv()
        slope_up.wait_recv()


def finish_kernel(cfg, act_in, score_in, got, got_slope, router_ref, act_out, score_out, up_out, up):
    def scoped(sems):
        count, cols = cfg["final_cuts"]
        copies = [pltpu.make_async_copy(act_in, act_out, sems.at[0]),
                  pltpu.make_async_copy(score_in, score_out, sems.at[1]),
                  pltpu.make_async_copy(up, up_out.at[0], sems.at[2])]
        for copy in copies[:2]:
            copy.start()
        scores_bf = got_slope[...].astype(BF)
        for c in range(count):
            span = pl.ds(c * cols, cols)
            term = lax.dot_general(
                scores_bf, router_ref[:, span], (((0,), (0,)), ((), ())), preferred_element_type=F32)
            token_grad = got[:, span].astype(F32) + term
            up[:, span] = token_grad.astype(BF)
            pltpu.make_async_copy(up.at[:, span], up_out.at[0, :, span], sems.at[2]).start()
        for copy in copies:
            copy.wait()

    pl.run_scoped(scoped, pltpu.SemaphoreType.DMA((3,)))


def on_device(grad_out, hidden_act, scores, expert_ids, slot_ids, counts, down_weight, router):
    n, n_section = lax.axis_size("expert"), lax.axis_size("section")
    _, tok, width = grad_out.shape
    hidden_width = hidden_act.shape[2]
    experts = scores.shape[2]
    capacity = max(2, 7 * tok // (4 * n))
    parts = row_parts(capacity)
    pieces = row_pieces(parts)
    cuts = [column_cuts(width, 7) for _ in parts]
    cfg = dict(n=n, n_section=n_section, parts=parts, pieces=pieces, cuts=cuts, weight_cuts=column_cuts(width, 7),
               final_cuts=column_cuts(width, 7))
    hbm = pl.BlockSpec(memory_space=pltpu.HBM)
    vmem = pl.BlockSpec(memory_space=pltpu.VMEM)
    scratch = [
        pltpu.VMEM((tok, width), BF),
        pltpu.VMEM((tok, hidden_width), BF),
        pltpu.VMEM((hidden_width, width), BF),
        pltpu.VMEM((experts, tok), F32),
        pltpu.VMEM((experts, tok), F32),
        pltpu.VMEM((1, tok), jnp.int32),
        pltpu.VMEM((1, tok), jnp.int32),
        pltpu.SMEM(counts.shape[1:], jnp.int32),
    ]
    scratch += [pltpu.VMEM((n, padded, width), BF) for _, _, padded in parts]
    scratch += [pltpu.VMEM((n, padded, width), BF) for _, _, padded in parts]
    scratch += [pltpu.VMEM((n * padded, hidden_width), F32) for _, _, padded in parts]
    scratch += [pltpu.VMEM((n, last - first, hidden_width), BF) for _, first, last in pieces]
    scratch += [pltpu.VMEM((n, last - first, hidden_width), BF) for _, first, last in pieces]
    scratch += [pltpu.VMEM((n * (last - first), hidden_width), F32) for _, first, last in pieces]
    kept = 2 * tok * (hidden_width + width) + 8 * tok * experts + 2 * experts * width
    vmem_limit = (67043328 - kept - 128 * 1024) // 4096 * 4096
    held = pl.pallas_call(
        functools.partial(kernel, cfg),
        out_shape=(
            pltpu.VMEM((1, tok, hidden_width), BF),
            pltpu.VMEM((1, experts, tok), F32),
            pltpu.VMEM((tok, width), BF),
            pltpu.VMEM((experts, tok), F32),
            pltpu.VMEM(router.shape, BF),
        ),
        in_specs=[hbm] * 8,
        out_specs=(vmem,) * 5,
        scratch_shapes=scratch,
        compiler_params=pltpu.CompilerParams(
            collective_id=0, has_side_effects=True, vmem_limit_bytes=vmem_limit),
    )(grad_out, hidden_act, jnp.swapaxes(scores, 1, 2), expert_ids, slot_ids, counts, down_weight, router)
    act_grad, score_grad, upstream = pl.pallas_call(
        functools.partial(finish_kernel, cfg),
        out_shape=(
            jax.ShapeDtypeStruct((1, tok, hidden_width), BF),
            jax.ShapeDtypeStruct((1, experts, tok), F32),
            jax.ShapeDtypeStruct((1, tok, width), BF),
        ),
        in_specs=[vmem] * 5,
        out_specs=(hbm,) * 3,
        scratch_shapes=[pltpu.VMEM((tok, width), BF)],
        compiler_params=pltpu.CompilerParams(vmem_limit_bytes=16 * 1024 * 1024),
    )(*held)
    return act_grad, jnp.swapaxes(score_grad, 1, 2), upstream


def solution(mesh):
    in_specs = (
        P("section", "expert", None),
        P("section", "expert", None),
        P("section", "expert", None),
        P("section", "expert"),
        P("section", "expert"),
        P("section", None, None),
        P("expert", None, None),
        P(),
    )
    out_specs = (
        P("section", "expert", None),
        P("section", "expert", None),
        P("section", "expert", None),
    )
    return jax.shard_map(
        on_device, mesh=mesh, in_specs=in_specs, out_specs=out_specs, check_vma=False
    )
```
